32 devices in a mesh: band: 16 (over z, y, core), grid: 2 (over x).
Axes of the slice: x: 2, y: 2, z: 4, core: 2. Of those that a mesh axis runs over, the one named last changes fastest.
Arguments:
- bands: float32 [32, 72, 5184], P('band', 'grid'), may hold values from -2.4 to 2.4
Outputs:
- exchange_terms: float32 [32, 72, 5184], P('band', 'grid')
The draws below stay inside these ranges and needn't reach their ends.
All inputs are finite; a program needn't handle non-finite values.
Results may differ from the reference program's by a relative error of at most 0.0001.
Values sent between devices are 32-bit elements; how exact they have to be, the bound alone decides.
No kernel may reach another device: no remote copies, remote signals or barrier semaphores. Data moves between devices by JAX's collectives and lax.ppermute only.
A program may use at most 128 MiB of HBM per device.

```python
import math
import jax
import jax.numpy as jnp
from jax import lax

GRID = 72
BAND_DEV = 2
STEPS = 3
BLOCKS = 16
BANDS = 32


def draw_bands(key, part):
    shape = (BANDS, GRID, GRID * GRID)
    return 0.4 * jax.random.truncated_normal(key, -6.0, 6.0, shape, jnp.float32)


def setup_inputs(seed: int = 0) -> dict:
    keys = jax.random.split(jax.random.key(seed), 2)
    return {
        "bands": draw_bands(jax.random.fold_in(keys[1], 71), 0),
    }


spacing = 0.5167


def tables(count):
    index = jnp.arange(count, dtype=jnp.int32)
    half = count // 2
    freq = jnp.where(index <= half, index, index - half)
    phase = ((freq[:, None] * index[None, :]) % count).astype(jnp.float32) * (2.0 * math.pi / count)
    table = jnp.where(index[:, None] <= half, jnp.cos(phase), jnp.sin(phase))
    weight = jnp.where((index == 0) | (index == half), 1.0, 2.0).astype(jnp.float32)
    square = freq.astype(jnp.float32) ** 2
    factor = (2.0 * math.pi / (count * spacing)) ** 2
    ksq = factor * (square[:, None, None] + square[None, :, None] + square[None, None, :])
    safe = jnp.where(ksq > 0, ksq, 1.0)
    coulomb = jnp.where(ksq > 0, 4.0 * math.pi / safe, 0.0)
    weights = weight[:, None, None] * weight[None, :, None] * weight[None, None, :]
    kernel = (coulomb * weights / float(count ** 3)).astype(jnp.float32)
    return table, kernel.reshape(count, count * count)


def forward_axis(values, table):
    return jnp.einsum('pmc,kc->pkm', values, table, precision=lax.Precision.HIGHEST)


def inverse_axis(values, table):
    return jnp.einsum('pmk,kr->prm', values, table, precision=lax.Precision.HIGHEST)


def coulomb_filter(density, table, kernel):
    count = table.shape[0]
    pairs = density.shape[0]
    work = forward_axis(density.reshape(pairs, count * count, count), table)
    work = forward_axis(work.reshape(pairs, count * count, count), table)
    work = forward_axis(work.reshape(pairs, count * count, count), table)
    work = work * kernel[None]
    work = inverse_axis(work.reshape(pairs, count * count, count), table)
    work = inverse_axis(work.reshape(pairs, count * count, count), table)
    work = inverse_axis(work.reshape(pairs, count * count, count), table)
    return work


def pair_terms(home, visit, table, kernel):
    home_count = home.shape[0]
    visit_count = visit.shape[0]
    count = home.shape[1]
    density = (home[:, None] * visit[None]).reshape(home_count * visit_count, count, home.shape[2])
    potential = coulomb_filter(density, table, kernel).reshape(home_count, visit_count, count, home.shape[2])
    home_part = -jnp.sum(potential * visit[None], axis=1)
    partner = -jnp.sum(potential * home[:, None], axis=0)
    return home_part, partner


def reference(bands):
    table, kernel = tables(GRID)
    blocks = bands.reshape(BLOCKS, BAND_DEV, GRID, GRID * GRID)
    total = jnp.zeros_like(blocks)
    for step in range(1, STEPS + 1):
        visiting = jnp.roll(blocks, step, axis=0)

        def one_block(pair):
            return pair_terms(pair[0], pair[1], table, kernel)

        home_part, partner = lax.map(one_block, (blocks, visiting))
        total = total + home_part + jnp.roll(partner, -step, axis=0)
    return total.reshape(bands.shape)
```

```python
import functools
import math

import jax
import jax.numpy as jnp
import numpy as np
from jax import lax
from jax.experimental import pallas as pl
from jax.experimental.pallas import tpu as pltpu
from jax.sharding import PartitionSpec as P

LANES = 128
SUB = 8
CHUNK = 36
spacing = 0.5167


def ceil_to(value, unit):
    return -(-value // unit) * unit


class Geometry:
    def __init__(self, count):
        self.count = count
        self.rows = count // 2
        self.full = self.rows // SUB
        self.rest = self.rows - self.full * SUB
        self.plane = count * count
        self.seg = ceil_to(self.plane, LANES)
        self.half = ceil_to(self.plane // 2, LANES)
        self.width = self.full * self.seg + self.half
        assert count % 2 == 0 and self.rest * 2 == SUB and count % SUB == 0 and count <= LANES
        self.positions = np.concatenate(
            [
                np.arange(self.full * SUB),
                self.full * SUB + np.arange(self.rest),
                self.rows + self.full * SUB + np.arange(self.rest),
                self.rows + np.arange(self.full * SUB),
            ]
        )


def table_of(count):
    index = np.arange(count)
    half = count // 2
    freq = np.where(index <= half, index, index - half)
    phase = (freq[:, None] * index[None, :] % count) * (2.0 * math.pi / count)
    return np.where(index[:, None] <= half, np.cos(phase), np.sin(phase))


def split(table):
    high = table.astype(np.float32).astype(jnp.bfloat16).astype(np.float32)
    return high, (table - high).astype(np.float32)


def lane_weight(table):
    count = table.shape[0]
    high, low = split(table)
    weight = np.zeros((2 * LANES, 2 * LANES), np.float32)
    for part in range(2):
        weight[part * LANES : part * LANES + count, :count] = high
        weight[part * LANES : part * LANES + count, LANES : LANES + count] = low
    return weight


def row_weight(table):
    high, low = split(table)
    return np.concatenate([high, high, low], 1)


def dot(left, right):
    return jnp.dot(left, right, preferred_element_type=jnp.float32)


def residue(values):
    return values - values.astype(jnp.bfloat16).astype(jnp.float32)


def lane_stage(values, weight):
    both = dot(jnp.concatenate([values, residue(values)], 1), weight)
    return both[:, :LANES] + both[:, LANES:]


def row_stage(weight, values):
    return dot(weight, jnp.concatenate([values, residue(values), values], 0))


def frequency(index, half):
    return jnp.where(index <= half, index, index - half).astype(jnp.float32)


def weighting(index, half):
    return jnp.where((index == 0) | (index == half), 1.0, 2.0)


def fill_kernel(count, kernel_ref):
    half = count // 2
    factor = (2.0 * math.pi / (count * spacing)) ** 2

    def body(first, carry):
        second = lax.broadcasted_iota(jnp.int32, (count, LANES), 0)
        third = lax.broadcasted_iota(jnp.int32, (count, LANES), 1)
        ksq = factor * (
            frequency(first, half) ** 2 + frequency(second, half) ** 2 + frequency(third, half) ** 2
        )
        weights = weighting(first, half) * weighting(second, half) * weighting(third, half)
        value = weights * (-4.0 * math.pi / float(count**3)) / jnp.where(ksq > 0, ksq, 1.0)
        kernel_ref[pl.ds(first * count, count), :] = jnp.where((ksq > 0) & (third < count), value, 0.0)
        return carry

    lax.fori_loop(0, count, body, 0)


def pair_filter(count, home_ref, visit_ref, kernel_ref, weights, work, other, emit):
    w3, w1, w2, v2, v1, v3 = weights

    def pairs(ref, at):
        return jnp.concatenate([ref[pl.ds(at + k, count, stride=count), :] for k in range(2)], 1)

    def forward(i, carry):
        at = i * (CHUNK * count)
        density = home_ref[pl.ds(at, CHUNK * count), :] * visit_ref[pl.ds(at, CHUNK * count), :]
        lines = lane_stage(density, w3[...])
        for u in range(0, CHUNK, 2):
            cut = [lines[(u + k) * count : (u + k + 1) * count] for k in range(2)]
            out = row_stage(w1[...], jnp.concatenate(cut, 1))
            for k in range(2):
                work[pl.ds(at + (u + k) * count, count), :] = out[:, k * LANES : (k + 1) * LANES]
        return carry

    def middle(i, carry):
        for u in range(0, CHUNK, 2):
            q = i * CHUNK + u
            out = row_stage(w2[...], pairs(work, q))
            scale = [kernel_ref[pl.ds((q + k) * count, count), :] for k in range(2)]
            back = row_stage(v2[...], out * jnp.concatenate(scale, 1))
            for k in range(2):
                other[pl.ds((q + k) * count, count), :] = back[:, k * LANES : (k + 1) * LANES]
        return carry

    def inverse(i, carry):
        lines = []
        for u in range(0, CHUNK, 2):
            out = row_stage(v1[...], pairs(other, i * CHUNK + u))
            lines += [out[:, :LANES], out[:, LANES:]]
        emit(i * (CHUNK * count), CHUNK * count, lane_stage(jnp.concatenate(lines, 0), v3[...]))
        return carry

    for part in (forward, middle, inverse):
        lax.fori_loop(0, count // CHUNK, part, 0)


def slot_body(geo, first_ref, second_ref, visit_ref, *rest):
    weights = rest[:6]
    first_out, second_out, partner_m, partner_r, kernel_ref, work, other, partner = rest[6:]
    fill_kernel(geo.count, kernel_ref)
    for order, (home_ref, out_ref) in enumerate(((first_ref, first_out), (second_ref, second_out))):

        def emit(at, rows, potential):
            out_ref[pl.ds(at, rows), :] = potential * visit_ref[pl.ds(at, rows), :]
            term = potential * home_ref[pl.ds(at, rows), :]
            if order:
                term = term + partner[pl.ds(at, rows), :]
            partner[pl.ds(at, rows), :] = term

        pair_filter(geo.count, home_ref, visit_ref, kernel_ref, weights, work, other, emit)
    to_messages(geo, (partner,), partner_m, partner_r)


def lane_index(rows=SUB):
    return lax.broadcasted_iota(jnp.int32, (rows, LANES), 1)


def upper_rows():
    return lax.broadcasted_iota(jnp.int32, (SUB, LANES), 0) < SUB // 2


def swap_halves(values):
    return jnp.concatenate([values[SUB // 2 :], values[: SUB // 2]], 0)


def cut_lines(tiles, lines, count, put):
    lane = lane_index()
    for j in range(lines):
        tile, shift = divmod(j * count, LANES)
        value = tiles(tile)
        if shift:
            value = pltpu.roll(value, LANES - shift, 1)
        if shift + count > LANES:
            value = jnp.where(lane < LANES - shift, value, pltpu.roll(tiles(tile + 1), LANES - shift, 1))
        put(j, jnp.where(lane < count, value, 0.0))


def join_lines(line, lines, count, put):
    lane = lane_index()
    for tile in range(-(-lines * count // LANES)):
        low = tile * LANES
        value = None
        for j in range(low // count, min(lines, -(-(low + LANES) // count))):
            shift = j * count - low
            piece = line(j)
            if shift % LANES:
                piece = pltpu.roll(piece, shift % LANES, 1)
            value = piece if value is None else jnp.where(lane < shift, value, piece)
        put(tile, value)


def from_messages(geo, mains, others, band_ref):
    count, seg = geo.count, geo.seg

    def read(refs, at):
        value = refs[0][:, pl.ds(at, LANES)]
        for ref in refs[1:]:
            value = value + ref[:, pl.ds(at, LANES)]
        return value

    for refs, base in ((mains, 0), (others, (geo.full + 1) * SUB)):

        def body(i, carry):
            def put(j, value):
                band_ref[pl.ds(pl.multiple_of(j * count + base + i * SUB, SUB), SUB), :] = value

            cut_lines(lambda tile: read(refs, pl.multiple_of(i * seg + tile * LANES, LANES)), count, count, put)
            return carry

        lax.fori_loop(0, geo.full, body, 0)
    at = geo.full * seg
    held = {}
    cut_lines(lambda tile: read(mains, at + tile * LANES), count // 2, count, lambda j, value: held.update({j: value}))

    def put(j, value):
        main = held.pop(j)
        low = j * count + geo.full * SUB
        high = (j + count // 2) * count + geo.full * SUB
        band_ref[low : low + SUB, :] = jnp.where(upper_rows(), main, swap_halves(value))
        band_ref[high : high + SUB, :] = jnp.where(upper_rows(), swap_halves(main), value)

    cut_lines(lambda tile: read(others, at + tile * LANES), count // 2, count, put)


def to_messages(geo, bands, main_ref, other_ref):
    count, seg = geo.count, geo.seg

    def read(at):
        value = bands[0][pl.ds(at, SUB), :]
        for ref in bands[1:]:
            value = value + ref[pl.ds(at, SUB), :]
        return value

    for ref, base in ((main_ref, 0), (other_ref, (geo.full + 1) * SUB)):

        def body(i, carry):
            def put(tile, value):
                ref[:, pl.ds(pl.multiple_of(i * seg + tile * LANES, LANES), LANES)] = value

            join_lines(lambda j: read(pl.multiple_of(j * count + base + i * SUB, SUB)), count, count, put)
            return carry

        lax.fori_loop(0, geo.full, body, 0)
    at = geo.full * seg

    def line(j, main):
        low = read(j * count + geo.full * SUB)
        high = read((j + count // 2) * count + geo.full * SUB)
        if main:
            return jnp.where(upper_rows(), low, swap_halves(high))
        return jnp.where(upper_rows(), swap_halves(low), high)

    for ref, main in ((main_ref, True), (other_ref, False)):

        def put(tile, value):
            ref[:, at + tile * LANES : at + (tile + 1) * LANES] = value

        join_lines(lambda j: line(j, main), count // 2, count, put)


def pack_body(geo, bands_ref, mine_ref, other_ref):
    grid = lax.axis_index("grid")
    for ref, band in ((mine_ref, grid), (other_ref, 1 - grid)):
        for i in range(geo.full):
            ref[:, i * geo.seg : i * geo.seg + geo.plane] = bands_ref[band, i * SUB : (i + 1) * SUB, :]
        at = geo.full * geo.seg
        low = bands_ref[band, geo.full * SUB :, : geo.plane // 2]
        high = bands_ref[band, geo.full * SUB :, geo.plane // 2 :]
        ref[:, at : at + geo.plane // 2] = jnp.concatenate([low, high], 0)


def finish_body(geo, mine_count, *refs):
    out_ref = refs[-1]
    mines, others = refs[:mine_count], refs[mine_count:-1]
    grid = lax.axis_index("grid")
    for parts, band in ((mines, grid), (others, 1 - grid)):

        def total(low, high):
            value = parts[0][:, low:high]
            for ref in parts[1:]:
                value = value + ref[:, low:high]
            return value

        for i in range(geo.full):
            out_ref[band, i * SUB : (i + 1) * SUB, :] = total(i * geo.seg, i * geo.seg + geo.plane)
        at = geo.full * geo.seg
        rest = total(at, at + geo.plane // 2)
        out_ref[band, geo.full * SUB :, : geo.plane // 2] = rest[: SUB // 2]
        out_ref[band, geo.full * SUB :, geo.plane // 2 :] = rest[SUB // 2 :]


def call(body, name, inputs, outputs, scratch=(), micros=2):
    whole = pl.BlockSpec(memory_space=pltpu.VMEM)
    return pl.pallas_call(
        body,
        out_shape=[jax.ShapeDtypeStruct(shape, jnp.float32) for shape in outputs],
        in_specs=[whole] * len(inputs),
        out_specs=[whole] * len(outputs),
        scratch_shapes=[pltpu.VMEM(shape, jnp.float32) for shape in scratch],
        compiler_params=pltpu.CompilerParams(vmem_limit_bytes=56 * 2**20),
        cost_estimate=pl.CostEstimate(
            flops=int(micros * 3e8), bytes_accessed=int(micros * 1e6), transcendentals=0
        ),
        name=name,
    )(*inputs)


def local(bands):
    rows, plane = bands.shape[1:]
    count = rows * lax.axis_size("grid")
    assert bands.shape[0] == lax.axis_size("grid") == 2 and plane == count * count
    geo = Geometry(count)
    devices = lax.axis_size("band")
    assert devices % 2 == 0
    grid = lax.axis_index("grid")
    message = (SUB, geo.width)
    band = (plane, LANES)

    def move(value, pairs):
        return lax.ppermute(value, "band", [(i % devices, j % devices) for i, j in pairs])

    def swap(value):
        return lax.ppermute(value, "grid", [(0, 1), (1, 0)])

    even = range(0, devices, 2)
    odd = range(1, devices, 2)
    across = [(i, i + 1) for i in even]
    back = [(i, i - 1) for i in odd]

    table = table_of(count)
    order = geo.positions
    both = np.stack([table[:, order], table[:, (order + rows) % count]])
    first = jnp.where(grid == 0, row_weight(both[0]), row_weight(both[1]))
    last = jnp.where(grid == 0, row_weight(both[0].T), row_weight(both[1].T))
    weights = [
        jnp.asarray(lane_weight(table.T)),
        first,
        jnp.asarray(row_weight(table)),
        jnp.asarray(row_weight(table.T)),
        last,
        jnp.asarray(lane_weight(table)),
    ]

    mine, other = call(functools.partial(pack_body, geo), "pack", [bands], [message] * 2)

    def entry(part):
        z = move(part, [(i, i + 3) for i in odd] + across)
        x = move(part, [(i, i + 1) for i in odd])
        y = move(part, [(i, i + 2) for i in even])
        return {"x": (x, move(x, across)), "y": (y, move(y, across)), "z": (z,)}

    def unpack(mains, others):
        def body(*refs):
            from_messages(geo, refs[: len(mains)], refs[len(mains) : -1], refs[-1])

        return call(body, "unpack", [*mains, *others], [band])[0]

    rest_mine = swap(other)
    rest_other = swap(mine)
    own_entry = entry(mine)
    rest_entry = entry(rest_mine)
    home_mine = unpack((mine,), (rest_mine,))
    home_other = unpack((other,), (rest_other,))
    slots = {}
    for name in ("x", "y", "z"):
        visit = unpack(own_entry[name], rest_entry[name])
        slots[name] = call(
            functools.partial(slot_body, geo),
            "slot",
            [home_other, home_mine, visit, *weights],
            [band, band, message, message],
            [band] * 4,
            micros=20,
        )

    def sum_bands(index):
        def body(*refs):
            to_messages(geo, refs[:3], refs[3], refs[4])

        return call(body, "join", [slots[name][index] for name in ("x", "y", "z")], [message] * 2)

    other_m, other_r = sum_bands(0)
    mine_m, mine_r = sum_bands(1)
    returned = []
    for part in (2, 3):
        x, y, z = (slots[name][part] for name in ("x", "y", "z"))
        back_x = move(x + move(x, back), [(i, i - 1) for i in even])
        back_y = move(y + move(y, back), [(i, i - 2) for i in even])
        back_z = move(z, [(i, i - 3) for i in even] + back)
        returned.append((back_x, back_y, back_z))
    from_other = swap(other_r)
    from_mine = swap(mine_r + returned[1][0] + returned[1][1] + returned[1][2])
    parts = [mine_m, *returned[0], from_other, other_m, from_mine]
    return call(functools.partial(finish_body, geo, 5), "finish", parts, [bands.shape])[0]


def solution(mesh):
    return jax.shard_map(
        local,
        mesh=mesh,
        in_specs=(P("band", "grid", None),),
        out_specs=P("band", "grid", None),
        check_vma=False,
    )
```

```python
import functools
import math

import jax
import jax.numpy as jnp
import numpy as np
from jax import lax
from jax.experimental import pallas as pl
from jax.experimental.pallas import tpu as pltpu
from jax.sharding import PartitionSpec as P


LANES = 128
SUB = 8
STEPS = 3
CHUNK = 72
spacing = 0.5167


def ceil_to(value, unit):
    return -(-value // unit) * unit


class Geometry:
    def __init__(self, count):
        self.count = count
        self.rows = count // 2
        self.full = self.rows // SUB
        self.rest = self.rows - self.full * SUB
        self.plane = count * count
        self.seg = ceil_to(self.plane, LANES)
        self.half = ceil_to(self.plane // 2, LANES)
        self.width = self.full * self.seg + self.half
        assert count % 2 == 0 and self.rest * 2 == SUB and count % SUB == 0 and count <= LANES
        self.positions = np.concatenate(
            [
                np.arange(self.full * SUB),
                self.full * SUB + np.arange(self.rest),
                self.rows + self.full * SUB + np.arange(self.rest),
                self.rows + np.arange(self.full * SUB),
            ]
        )


def table_of(rows, columns, count):
    half = count // 2
    freq = jnp.where(rows <= half, rows, rows - half)
    phase = (freq * columns % count).astype(jnp.float32) * (2.0 * math.pi / count)
    return jnp.where(rows <= half, jnp.cos(phase), jnp.sin(phase))


def split(table):
    high = table.astype(jnp.bfloat16).astype(jnp.float32)
    return high, table - high


def dot(left, right):
    return jnp.dot(left, right, preferred_element_type=jnp.float32)


def residue(values):
    return values - values.astype(jnp.bfloat16).astype(jnp.float32)


def lane_stage(values, weight):
    both = dot(jnp.concatenate([values, residue(values)], 1), weight)
    return both[:, :LANES] + both[:, LANES:]


def row_stage(weight, values):
    return dot(weight, jnp.concatenate([values, residue(values), values], 0))


def frequency(index, half):
    return jnp.where(index <= half, index, index - half).astype(jnp.float32)


def weighting(index, half):
    return jnp.where((index == 0) | (index == half), 1.0, 2.0)


def fill_kernel(count, kernel_ref):
    half = count // 2
    factor = (2.0 * math.pi / (count * spacing)) ** 2

    def body(first, carry):
        second = lax.broadcasted_iota(jnp.int32, (count, LANES), 0)
        third = lax.broadcasted_iota(jnp.int32, (count, LANES), 1)
        ksq = factor * (
            frequency(first, half) ** 2 + frequency(second, half) ** 2 + frequency(third, half) ** 2
        )
        weights = weighting(first, half) * weighting(second, half) * weighting(third, half)
        value = weights * (-4.0 * math.pi / float(count**3)) / jnp.where(ksq > 0, ksq, 1.0)
        kernel_ref[pl.ds(first * count, count), :] = jnp.where((ksq > 0) & (third < count), value, 0.0)
        return carry

    lax.fori_loop(0, count, body, 0)


def offset_of(geo, line):
    return line * geo.count % LANES


def place_rows(weight, start):
    count = weight.shape[0]
    zeros = jnp.zeros((LANES - count, weight.shape[1]), jnp.float32)
    if start + count <= LANES:
        lanes = [zeros[:start], weight, zeros[start:]]
    else:
        lanes = [weight[LANES - start :], zeros, weight[: LANES - start]]
    return jnp.concatenate([part for part in lanes if part.shape[0]] * 2, 0)


def lane_index():
    return lax.broadcasted_iota(jnp.int32, (SUB, LANES), 1)


def upper_rows():
    return lax.broadcasted_iota(jnp.int32, (SUB, LANES), 0) < SUB // 2


def swap_halves(values):
    return jnp.concatenate([values[SUB // 2 :], values[: SUB // 2]], 0)


def pair_body(geo, extra, sum_home, sum_partner, *refs):
    refs = list(refs)

    def take(number):
        taken = refs[:number]
        del refs[:number]
        return taken

    count, full = geo.count, geo.full
    seg, half = geo.seg // LANES, count // 2
    home, visit = take(2), take(2)
    added = take(2) if extra else None
    home_in = take(2) if sum_home else None
    partner_in = take(2) if sum_partner else None
    factor, w3, w1, w2, v2, v1, v3 = take(7)
    home_out, partner_out = take(2), take(2)
    work, other = take(2)
    if extra:
        sums = take(2)
        for part in range(2):
            sums[part][...] = visit[part][...] + added[part][...]
        visit = sums
    lane, upper = lane_index(), upper_rows()
    period = LANES // SUB

    def cell(ref, tile):
        return ref[:, tile * LANES : (tile + 1) * LANES]

    def density(part, base, line):
        tile, shift = divmod(line * count, LANES)
        tile += base
        value = cell(home[part], tile) * cell(visit[part], tile)
        if shift + count > LANES:
            value = jnp.where(lane >= shift, value, cell(home[part], tile + 1) * cell(visit[part], tile + 1))
        return value

    def spot(line, tile):
        return pl.ds(line * count + tile * SUB, SUB)

    bases = [(part, i * seg, i + part * (full + 1)) for part in range(2) for i in range(full)]

    def put_lines(ref, lines, out):
        for k, line in enumerate(lines):
            ref[pl.ds(line * count, count), :] = out[:, k * LANES : (k + 1) * LANES]

    for c in range(period):
        lines, locals_ = range(c, count, period), range(c, half, period)
        cells = [density(part, base, line) for line in lines for part, base, _ in bases]
        cells += [density(part, full * seg, line) for line in locals_ for part in range(2)]
        out = lane_stage(jnp.concatenate(cells, 0), place_rows(w3[...], offset_of(geo, c)))
        pieces = iter([out[k * SUB : (k + 1) * SUB] for k in range(len(cells))])
        for line in lines:
            for _, _, tile in bases:
                other[spot(line, tile), :] = next(pieces)
        for line in locals_:
            main, rest = next(pieces), next(pieces)
            other[spot(line, full), :] = jnp.where(upper, main, swap_halves(rest))
            other[spot(line + half, full), :] = jnp.where(upper, swap_halves(main), rest)

    for line in range(0, count, 2):
        cut = [other[pl.ds((line + k) * count, count), :] for k in range(2)]
        put_lines(work, (line, line + 1), row_stage(w1[...], jnp.concatenate(cut, 1)))

    def spread(ref, lines):
        return jnp.concatenate([ref[pl.ds(line, count, stride=count), :] for line in lines], 1)

    def middle(i, carry):
        for u in range(0, CHUNK, 2):
            q = i * CHUNK + u
            out = row_stage(w2[...], spread(work, (q, q + 1)))
            scale = [factor[pl.ds((q + k) * count, count), :] for k in range(2)]
            put_lines(other, (q, q + 1), row_stage(v2[...], out * jnp.concatenate(scale, 1)))
        return carry

    lax.fori_loop(0, count // CHUNK, middle, 0)

    for line in range(0, count, 2):
        put_lines(work, (line, line + 1), row_stage(v1[...], spread(other, (line, line + 1))))

    for c in range(period):
        lines, locals_ = range(c, count, period), range(c, half, period)
        cells = [work[spot(line, tile), :] for line in lines for _, _, tile in bases]
        for line in locals_:
            low, high = work[spot(line, full), :], work[spot(line + half, full), :]
            cells += [jnp.where(upper, low, swap_halves(high)), jnp.where(upper, swap_halves(low), high)]
        out = lane_stage(jnp.concatenate(cells, 0), place_rows(v3[c * count : (c + 1) * count, :], 0))
        pieces = iter([out[k * SUB : (k + 1) * SUB] for k in range(len(cells))])
        for line in lines:
            for _, _, tile in bases:
                work[spot(line, tile), :] = next(pieces)
        for line in locals_:
            for part in range(2):
                work[spot(line + part * half, full), :] = next(pieces)

    def emit(part, base, lines, line_of):
        for tile in range(-(-lines * count // LANES)):
            low = tile * LANES
            value = None
            for line in range(low // count, min(lines, -(-(low + LANES) // count))):
                piece = work[line_of(line), :]
                value = piece if value is None else jnp.where(lane < line * count - low, value, piece)
            at = pl.ds(base + low, LANES)
            for ins, outs, factors in ((home_in, home_out, visit), (partner_in, partner_out, home)):
                term = value * factors[part][:, at]
                outs[part][:, at] = term if ins is None else ins[part][:, at] + term

    for part in range(2):

        def segment(i, carry):
            row = (i + part * (full + 1)) * SUB
            emit(
                part,
                pl.multiple_of(i * seg * LANES, LANES),
                count,
                lambda line: pl.ds(pl.multiple_of(line * count + row, SUB), SUB),
            )
            return carry

        lax.fori_loop(0, full, segment, 0)
        emit(part, full * seg * LANES, half, lambda line: spot(line + part * half, full))


def factor_body(geo, tables, back_tables, factor_ref, w3, w1, w2, v2, v1, v3):
    count = geo.count
    fill_kernel(count, factor_ref)
    for source, index, ref in ((tables, 0, w2), (tables, 1, w1), (back_tables, 0, v2), (back_tables, 1, v1)):
        high, low = split(source[index])
        ref[...] = jnp.concatenate([high, high, low], 1)
    blank = jnp.zeros((count, LANES - count), jnp.float32)
    for part, value in enumerate(split(back_tables[0])):
        w3[:, part * LANES : (part + 1) * LANES] = jnp.concatenate([value, blank], 1)
    for part, value in enumerate(split(tables[0])):
        value = jnp.concatenate([value, blank], 1)
        for c in range(LANES // SUB):
            shift = offset_of(geo, c)
            placed = pltpu.roll(value, shift, 1) if shift else value
            v3[c * count : (c + 1) * count, part * LANES : (part + 1) * LANES] = placed


def padded(values, width):
    return jnp.concatenate([values, jnp.zeros((values.shape[0], width - values.shape[1]), jnp.float32)], 1)


def pack_body(geo, bands_ref, mine_ref, other_ref):
    grid = lax.axis_index("grid")
    for ref, band in ((mine_ref, grid), (other_ref, 1 - grid)):
        for i in range(geo.full):
            rows = bands_ref[band, i * SUB : (i + 1) * SUB, :]
            ref[:, i * geo.seg : (i + 1) * geo.seg] = padded(rows, geo.seg)
        at = geo.full * geo.seg
        low = bands_ref[band, geo.full * SUB :, : geo.plane // 2]
        high = bands_ref[band, geo.full * SUB :, geo.plane // 2 :]
        ref[:, at : at + geo.half] = padded(jnp.concatenate([low, high], 0), geo.half)


def finish_body(geo, mine_count, *refs):
    out_ref = refs[-1]
    mines, others = refs[:mine_count], refs[mine_count:-1]
    grid = lax.axis_index("grid")
    for parts, band in ((mines, grid), (others, 1 - grid)):

        def total(low, high):
            value = parts[0][:, low:high]
            for ref in parts[1:]:
                value = value + ref[:, low:high]
            return value

        for i in range(geo.full):
            out_ref[band, i * SUB : (i + 1) * SUB, :] = total(i * geo.seg, i * geo.seg + geo.plane)
        at = geo.full * geo.seg
        rest = total(at, at + geo.plane // 2)
        out_ref[band, geo.full * SUB :, : geo.plane // 2] = rest[: SUB // 2]
        out_ref[band, geo.full * SUB :, geo.plane // 2 :] = rest[SUB // 2 :]


def call(body, inputs, outputs, scratch=(), micros=2):
    whole = pl.BlockSpec(memory_space=pltpu.VMEM)
    return pl.pallas_call(
        body,
        out_shape=[jax.ShapeDtypeStruct(shape, jnp.float32) for shape in outputs],
        in_specs=[whole] * len(inputs),
        out_specs=[whole] * len(outputs),
        scratch_shapes=[pltpu.VMEM(shape, jnp.float32) for shape in scratch],
        compiler_params=pltpu.CompilerParams(vmem_limit_bytes=24 * 2**20),
        cost_estimate=pl.CostEstimate(
            flops=int(micros * 3e8), bytes_accessed=int(micros * 1e6), transcendentals=0
        ),
    )(*inputs)


def local(bands):
    rows, plane = bands.shape[1:]
    count = rows * lax.axis_size("grid")
    assert bands.shape[0] == lax.axis_size("grid") == 2 and plane == count * count
    geo = Geometry(count)
    devices = lax.axis_size("band")
    assert devices % 2 == 0
    grid = lax.axis_index("grid")
    message = (SUB, geo.width)
    band = (plane, LANES)

    def move(value, pairs):
        return lax.ppermute(value, "band", [(i % devices, j % devices) for i, j in pairs])

    def swap(value):
        return lax.ppermute(value, "grid", [(0, 1), (1, 0)])

    even = range(0, devices, 2)
    odd = range(1, devices, 2)
    every = range(devices)
    across = [(i, i + 1) for i in even]
    back = [(i, i - 1) for i in odd]

    mine, other = call(functools.partial(pack_body, geo), [bands], [message] * 2)
    index = jnp.arange(count, dtype=jnp.int32)
    cells = jnp.stack([index, (jnp.asarray(geo.positions, jnp.int32) + rows * grid) % count])
    tables = table_of(index[None, :, None], cells[:, None, :], count)
    back_tables = table_of(index[None, None, :], cells[:, :, None], count)
    wide, tall = (count, 2 * LANES), (count, 3 * count)
    factor, *weights = call(
        functools.partial(factor_body, geo),
        [tables, back_tables],
        [band, wide, *[tall] * 4, (count * (LANES // SUB), 2 * LANES)],
    )

    def entry(part):
        one = move(part, [(i, i + 1) for i in every])
        two = move(part, [(i, i + 2) for i in even])
        three = move(part, [(i, i + 3) for i in odd])
        return (one,), (two, move(one, across)), (three, move(two, across))

    rest_mine = swap(other)
    rest_other = swap(mine)
    visits = list(zip(entry(mine), entry(rest_mine)))
    homes = {"other": (other, rest_other), "mine": (mine, rest_mine)}
    sums = {"other": None, "mine": None}
    partners = [None] * STEPS
    for name, step in PAIRS:
        parts = visits[step - 1]
        visit = [part[k] for k in range(len(parts[0])) for part in parts]
        home_in, partner_in = sums[name], partners[step - 1]
        out = call(
            functools.partial(
                pair_body, geo, len(visit) > 2, home_in is not None, partner_in is not None
            ),
            [*homes[name], *visit, *(home_in or ()), *(partner_in or ()), factor, *weights],
            [message] * 4,
            [band] * 2 + ([message] * 2 if len(visit) > 2 else []),
            micros=8,
        )
        sums[name], partners[step - 1] = out[:2], out[2:]
    other_m, other_r = sums["other"]
    mine_m, mine_r = sums["mine"]
    one, two, three = partners

    def shared(step, part):
        return move(partners[step - 1][part], back)

    rest = [
        move(one[1] + shared(2, 1), [(i, i - 1) for i in every]),
        move(two[1] + shared(3, 1), [(i, i - 2) for i in even]),
        move(three[1], [(i, i - 3) for i in even]),
    ]
    main = [
        move(one[0] + shared(2, 0), [(i, i - 1) for i in every]),
        move(two[0] + shared(3, 0), [(i, i - 2) for i in even]),
        move(three[0], [(i, i - 3) for i in even]),
    ]
    from_other = swap(other_r)
    from_mine = swap(mine_r + rest[0] + rest[1] + rest[2])
    parts = [mine_m, *main, from_other, other_m, from_mine]
    return call(functools.partial(finish_body, geo, 5), parts, [bands.shape])[0]


PAIRS = (("mine", 1), ("other", 1), ("other", 2), ("mine", 2), ("other", 3), ("mine", 3))


def solution(mesh):
    return jax.shard_map(
        local,
        mesh=mesh,
        in_specs=(P("band", "grid", None),),
        out_specs=P("band", "grid", None),
        check_vma=False,
    )
```
